128 devices in a mesh: row: 2 (over core), col: 2 (over x_hi), depth: 32 (over z, y, x_lo).
Axes of the slice: x: 4 (x_hi: 2, x_lo: 2; x = x_hi * 2 + x_lo), y: 4, z: 4, core: 2. Of those that a mesh axis runs over, the one named last changes fastest.
Arguments:
- a_blocks: bfloat16 [64, 128, 4096], P('row', ('col', 'depth')), may hold values from -6 to 6
- a_mask: int32 [64, 128], P('row', ('col', 'depth')), may hold values 0 or 1
- a_row_ids: int32 [64], replicated, may hold values from 0 to 63, as said below
- a_col_ids: int32 [128], replicated, may hold values from 0 to 127, as said below
- b_matrix: bfloat16 [8192, 6144], P(('row', 'depth'), 'col'), may hold values from -0.0625 to 0.0625
- b_mask: int32 [128, 96], P(('row', 'depth'), 'col'), may hold values 0 or 1
Outputs:
- product: bfloat16 [4096, 6144], P(('row', 'depth'), 'col')
The draws below stay inside these ranges and needn't reach their ends.
Inputs may be any that keep to these rules, and one draw needn't show every extreme that they name: `a_row_ids`: A permutation of the block rows; each aligned set of 32 entries holds at most 17 block rows r with the same r // 32, and every draw reaches 17. `a_col_ids`: A permutation of the block columns; entry v holds a block column k with (k // 2) % 32 == (v // 2) % 32.
All inputs are finite; a program needn't handle non-finite values. No bound on the sum of `a_mask` or of `b_mask` on one device may be relied on, other than what follows from the above.
Results may differ from the reference program's by a relative error of at most 0.001.
Values may be sent and summed in bfloat16 or wider, within the bound.
A program may use at most 64 MiB of HBM per device.

```python
import jax
import jax.numpy as jnp
from jax import lax

BLOCK = 64
BAS = 8192
NV = 6144
ROWS = 4096
NBR = 64
RB = 32
KBLK = 128
KC = 2


def draw_a_row_ids(key, part):
    grid_size = NBR // RB
    spread = RB // grid_size
    first_key, second_key, third_key = jax.random.split(key, 3)
    gaining = jax.random.permutation(first_key, grid_size).astype(jnp.int32)
    losing = jnp.roll(gaining, -1)
    positions = jnp.arange(RB, dtype=jnp.int32)
    labels = jnp.where(positions[None, :] == losing[:, None] * spread, gaining[:, None], (positions // spread)[None, :])
    mixing = jax.vmap(lambda single: jax.random.permutation(single, RB))(jax.random.split(second_key, grid_size)).astype(jnp.int32)
    labels = jnp.take_along_axis(labels, mixing, axis=1).reshape(-1)
    tiebreak = jax.random.permutation(third_key, NBR).astype(jnp.int32)
    ranking = jnp.argsort(labels * NBR + tiebreak, stable=True).astype(jnp.int32)
    return jnp.zeros((NBR,), jnp.int32).at[ranking].set(jnp.arange(NBR, dtype=jnp.int32))


def draw_a_col_ids(key, part):
    grid_size = NBR // RB
    planes = KBLK // (KC * grid_size)
    members = grid_size * KC
    first_key, second_key = jax.random.split(key, 2)
    shuffles = jax.vmap(lambda single: jax.random.permutation(single, members))(jax.random.split(first_key, planes)).astype(jnp.int32)
    chosen = jax.random.randint(second_key, (), 0, planes)
    shuffles = jnp.where(jnp.arange(planes, dtype=jnp.int32)[:, None] == chosen, jnp.arange(members, dtype=jnp.int32)[None, :], shuffles)
    column = jnp.arange(KBLK, dtype=jnp.int32)
    shard_of = column // KC
    plane_of = shard_of % planes
    holder = shard_of // planes
    picked = shuffles[plane_of, holder * KC + column % KC]
    return ((picked // KC * planes + plane_of) * KC + picked % KC).astype(jnp.int32)


def plant(entries, rng, least, high):
    shape = entries.shape
    place = [jax.random.randint(jax.random.fold_in(rng, axis), (), 0, shape[axis]) for axis in range(len(shape))]
    entries = entries.at[tuple(place)].set(least)
    longest = shape.index(max(shape))
    place[longest] = (place[longest] + 1) % shape[longest]
    return entries.at[tuple(place)].set(high)


def levels(rng, shape, cuts, smallest, top_value):
    factor_of = 1.0
    for axis_at, shards_of in cuts:
        steps = jax.random.uniform(jax.random.fold_in(jax.random.fold_in(rng, 6), axis_at), (shards_of,), jnp.float32, smallest / len(cuts), top_value / len(cuts))
        factor_of = factor_of * jnp.repeat(jnp.exp(steps), shape[axis_at] // shards_of).reshape((-1,) + (1,) * (len(shape) - 1 - axis_at))
    return factor_of


def noise(rng, dims, scale, bound, cuts=(), held_as=jnp.bfloat16):
    loudness = levels(rng, dims, cuts, -0.22, 0.18) if cuts else 1.0
    entries = jax.random.normal(rng, dims, jnp.float32) * scale * loudness
    return jnp.minimum(jnp.maximum(entries, -bound), bound).astype(held_as)


def setup_inputs(seed: int = 0) -> dict:
    splits = jax.random.split(jax.random.key(seed), 7)
    a_blocks = noise(splits[0], (NBR, KBLK, BLOCK * BLOCK), 1.0, 6.0, ((0, 2), (1, 64)))
    a_mask = plant((jax.random.randint(splits[1], (NBR, KBLK), 0, 4) < 3).astype(jnp.int32), jax.random.fold_in(splits[1], 1), 0, 1)
    a_row_ids = draw_a_row_ids(jax.random.fold_in(splits[6], 71), 0)
    a_col_ids = draw_a_col_ids(jax.random.fold_in(splits[6], 71), 0)
    b_matrix = noise(splits[4], (BAS, NV), BAS ** -0.5, 0.0625, ((0, 64), (1, 2)))
    b_mask = plant((jax.random.randint(splits[5], (KBLK, NV // BLOCK), 0, 4) < 3).astype(jnp.int32), jax.random.fold_in(splits[5], 1), 0, 1)
    return {"a_blocks": a_blocks, "a_mask": a_mask, "a_row_ids": a_row_ids, "a_col_ids": a_col_ids, "b_matrix": b_matrix, "b_mask": b_mask}


def reference(a_blocks, a_mask, a_row_ids, a_col_ids, b_matrix, b_mask):
    row_slot = jnp.zeros((NBR,), jnp.int32).at[a_row_ids].set(jnp.arange(NBR, dtype=jnp.int32))
    col_slot = jnp.zeros((KBLK,), jnp.int32).at[a_col_ids].set(jnp.arange(KBLK, dtype=jnp.int32))
    masked = a_blocks * a_mask[:, :, None].astype(a_blocks.dtype)
    ordered = masked[row_slot][:, col_slot]
    left_matrix = ordered.reshape(NBR, KBLK, BLOCK, BLOCK).transpose(0, 2, 1, 3).reshape(ROWS, BAS)
    right_matrix = b_matrix.reshape(KBLK, BLOCK, NV // BLOCK, BLOCK) * b_mask[:, None, :, None].astype(b_matrix.dtype)
    right_matrix = right_matrix.reshape(BAS, NV)
    product = jnp.dot(left_matrix.astype(jnp.float32), right_matrix.astype(jnp.float32), precision=lax.Precision.HIGHEST)
    return product.astype(jnp.bfloat16)
```

```python
import functools

import jax
import jax.numpy as jnp
from jax import lax
from jax.experimental import pallas as pl
from jax.experimental.pallas import tpu as pltpu
from jax.sharding import PartitionSpec as P

MESH = pl.DeviceIdType.MESH
CHUNKS = (384, 384, 384, 384)
GROUPS = ((2,), (1, 3), (0,))
HALF = 1536
F32 = jnp.float32
BF16 = jnp.bfloat16


def kernel(
    slot_ref, colid_ref, amask_ref, bmask_ref, a_ref, b_ref, out_ref,
    araw, tmp, bxs, pst, abuf, bbuf, rbuf, cp, rsin, rsout, rsfin, ilv, fin_s, fin_r,
    sx_s, sx_r, sa_s, sa_r, sb_s, sb_r, sc_s, sc_r,
):
    r = lax.axis_index("row")
    c = lax.axis_index("col")
    d = lax.axis_index("depth")
    z = lax.div(d, 8)
    y = lax.rem(lax.div(d, 2), 4)
    l = lax.rem(d, 2)
    x = c * 2 + l

    def depth_of(zz, yy, ll):
        return zz * 8 + yy * 2 + ll

    def dev_y(k):
        return (r, c, depth_of(z, lax.rem(y + k, 4), l))

    def dev_z(k):
        return (r, c, depth_of(lax.rem(z + k, 4), y, l))

    def dev_x(k):
        xx = lax.rem(x + k, 4)
        return (r, lax.div(xx, 2), depth_of(z, y, lax.rem(xx, 2)))

    sib = (1 - r, c, d)
    part = (r, c, depth_of(z, y, 1 - l))

    pending = []

    def rcopy(src, dst, ss, rs, dev):
        copy = pltpu.make_async_remote_copy(
            src_ref=src, dst_ref=dst, send_sem=ss, recv_sem=rs, device_id=dev, device_id_type=MESH
        )
        copy.start()
        pending.append(copy)
        return copy

    barrier = pltpu.get_barrier_semaphore()
    peers = [dev_y(1), dev_y(2), dev_y(3), dev_z(1), dev_z(3), dev_x(1), dev_x(3), sib]
    for peer in peers:
        pl.semaphore_signal(barrier, inc=1, device_id=peer, device_id_type=MESH)

    odd = lax.rem(lax.broadcasted_iota(jnp.int32, (64, 128), 0), 2) == 1

    def mask_a(u, _):
        factor = jnp.where(odd, amask_ref[1, u], amask_ref[0, u]).astype(F32)
        araw[r * 32 + u] = (a_ref[u].astype(F32) * factor).astype(BF16)
        return 0

    lax.fori_loop(0, 32, mask_a, 0, unroll=4)

    pl.semaphore_wait(barrier, len(peers))
    mine = pl.ds(r * 32, 32)
    ax = rcopy(araw.at[mine], araw.at[mine], sx_s, sx_r, sib)

    own_plane = y * 2 + l
    left_lane = lax.broadcasted_iota(jnp.int32, (64, 128), 1) < 64

    def mask_b(ch, half):
        start = sum(CHUNKS[:ch])
        for j in range(2):
            for t in range(CHUNKS[ch] // 128):
                col = half * HALF + (start + t * 128)
                block = half * (HALF // 64) + (start // 64 + t * 2)
                factor = jnp.where(left_lane, bmask_ref[j, block], bmask_ref[j, block + 1]).astype(F32)
                tile = b_ref[pl.ds(j * 64, 64), pl.ds(pl.multiple_of(col, 128), 128)].astype(F32)
                yield j, t, (tile * factor).astype(BF16)

    def prep_own(ch):
        for j, t, tile in mask_b(ch, l):
            bbuf[ch][own_plane, r * 2 + j, :, pl.ds(t * 128, 128)] = tile

    def prep_other(ch):
        for j, t, tile in mask_b(ch, 1 - l):
            bxs[ch][j, :, pl.ds(t * 128, 128)] = tile

    two = pl.ds(r * 2, 2)

    def piece(ch, k, lam):
        plane = lax.rem(y + k, 4) * 2 + (l if lam == 0 else 1 - l)
        return bbuf[ch].at[plane, two]

    B = {}

    def b_copy(ch, i, ref, dev):
        B[ch, i] = rcopy(ref, ref, sb_s.at[ch, i], sb_r.at[ch, i], dev)

    def b_pair(ch):
        B[ch, 0] = rcopy(bxs[ch], bbuf[ch].at[own_plane, two], sb_s.at[ch, 0], sb_r.at[ch, 0], part)

    def b_own(ch):
        b_copy(ch, 1, piece(ch, 0, 0), dev_y(1))
        b_copy(ch, 4, piece(ch, 0, 0), dev_y(3))

    def b_own_sib(ch):
        b_copy(ch, 7, piece(ch, 0, 0), sib)

    def b_other(ch):
        B[ch, 0].wait_recv()
        b_copy(ch, 2, piece(ch, 0, 1), dev_y(1))
        b_copy(ch, 5, piece(ch, 0, 1), dev_y(3))
        b_copy(ch, 8, piece(ch, 0, 1), sib)

    def b_mid(ch):
        B[ch, 1].wait_recv()
        b_copy(ch, 3, piece(ch, 3, 0), dev_y(1))
        b_copy(ch, 9, piece(ch, 3, 0), sib)
        B[ch, 4].wait_recv()
        b_copy(ch, 10, piece(ch, 1, 0), sib)
        B[ch, 5].wait_recv()
        b_copy(ch, 6, piece(ch, 1, 1), dev_y(3))
        b_copy(ch, 11, piece(ch, 1, 1), sib)
        B[ch, 2].wait_recv()
        b_copy(ch, 12, piece(ch, 3, 1), sib)

    def b_far(ch):
        B[ch, 3].wait_recv()
        b_copy(ch, 13, piece(ch, 2, 0), sib)
        B[ch, 6].wait_recv()
        b_copy(ch, 14, piece(ch, 2, 1), sib)

    def b_ready(ch):
        for i in range(7, 15):
            B[ch, i].wait_recv()
        for plane in range(8):
            for cc in range(2):
                for jj in range(2):
                    stored = (cc * 32 + z * 8 + plane) * 2 + jj
                    k = colid_ref[stored]
                    sel = lax.div(k, 64) * 2 + lax.rem(k, 2)
                    rbuf[ch][pl.ds((plane * 4 + cc * 2 + jj) * 64, 64), :] = bbuf[ch][plane, sel]

    def source(xx, yy):
        return (yy * 2 + lax.rem(xx, 2)) * 2 + lax.div(xx, 2)

    A = {}

    def a_copy(g, i, src, dst, dev):
        A[g, i] = rcopy(src, dst, sa_s.at[g, i], sa_r.at[g, i], dev)

    def a_prep(g):
        for k in (2, 1, 3, 0):
            yy = lax.rem(y + k, 4)
            n = 0
            for zr in GROUPS[g]:
                zz = lax.rem(z + zr, 4)
                for ll in range(2):
                    u = slot_ref[r * 32 + zz * 8 + yy * 2 + ll]
                    slot = (k * 8 + n) % 8
                    tmp[slot] = araw[u].astype(F32)
                    first = tmp[slot, pl.ds(0, 32, stride=2), :]
                    second = tmp[slot, pl.ds(1, 32, stride=2), :]
                    lane = left_lane[:32]
                    even = jnp.where(lane, first, pltpu.roll(second, 64, 1))
                    oddr = jnp.where(lane, pltpu.roll(first, 64, 1), second)
                    block = jnp.concatenate([even, oddr], axis=0).astype(BF16)
                    if k == 0:
                        abuf[g][source(x, y), pl.ds(n * 64, 64), :] = block
                    else:
                        pst[g][k - 1, pl.ds(n * 64, 64), :] = block
                    n += 1
            if k:
                a_copy(g, k - 1, pst[g].at[k - 1], abuf[g].at[source(x, y)], dev_y(k))
            else:
                a_ring(g, 0)

    def a_ring(g, k):
        if k:
            A[g, k - 1].wait_recv()
        ref = abuf[g].at[source(x, lax.rem(y + 4 - k, 4))]
        a_copy(g, 3 + k, ref, ref, dev_x(1))
        a_copy(g, 7 + k, ref, ref, dev_x(3))

    def a_rest(g):
        for k in (1, 3, 2):
            a_ring(g, k)

    def a_forward(g):
        for i, k in enumerate((0, 1)):
            A[g, 3 + k].wait_recv()
            ref = abuf[g].at[source(lax.rem(x + 3, 4), lax.rem(y + 4 - k, 4))]
            a_copy(g, 11 + i, ref, ref, dev_x(1))
        for i, k in enumerate((3, 2)):
            A[g, 7 + k].wait_recv()
            ref = abuf[g].at[source(lax.rem(x + 1, 4), lax.rem(y + 4 - k, 4))]
            a_copy(g, 13 + i, ref, ref, dev_x(3))

    def a_ready(g):
        for i in (5, 6, 7, 8, 11, 12, 13, 14):
            A[g, i].wait_recv()

    def multiply(ch, zr):
        g = [n for n, group in enumerate(GROUPS) if zr in group][0]
        rows = pl.ds(GROUPS[g].index(zr) * 128, 128)
        lhs = jnp.concatenate([abuf[g][i, rows, :] for i in range(16)], axis=1)
        total = jnp.dot(lhs, rbuf[ch][...], preferred_element_type=F32)
        cp[ch][zr, 0] = total[:64]
        cp[ch][zr, 1] = total[64:]

    C = {}

    def c_copy(ch, i, src, dst, dev):
        C[ch, i] = rcopy(src, dst, sc_s.at[ch, i], sc_r.at[ch, i], dev)

    def c_far(ch):
        multiply(ch, 2)
        c_copy(ch, 0, cp[ch].at[2, 0], rsin[ch].at[0], dev_z(1))
        c_copy(ch, 1, cp[ch].at[2, 1], rsin[ch].at[1], dev_z(3))

    def c_near(ch):
        multiply(ch, 1)
        c_copy(ch, 2, cp[ch].at[1, 1], rsin[ch].at[2], dev_z(1))
        multiply(ch, 3)
        c_copy(ch, 3, cp[ch].at[3, 0], rsin[ch].at[3], dev_z(3))

    def c_combine(ch):
        C[ch, 0].wait_recv()
        rsout[ch][0] = rsin[ch][0] + cp[ch][1, 0]
        c_copy(ch, 4, rsout[ch].at[0], rsfin[ch].at[0], dev_z(1))
        C[ch, 1].wait_recv()
        rsout[ch][1] = rsin[ch][1] + cp[ch][3, 1]
        c_copy(ch, 5, rsout[ch].at[1], rsfin[ch].at[1], dev_z(3))

    def c_own(ch):
        multiply(ch, 0)

    def columns(ch, half):
        return pl.ds(pl.multiple_of(half * HALF + sum(CHUNKS[:ch]), 128), CHUNKS[ch])

    def c_final(ch):
        C[ch, 3].wait_recv()
        C[ch, 4].wait_recv()
        value = cp[ch][0, 0] + rsin[ch][3] + rsfin[ch][0]
        for t in range(CHUNKS[ch] // 128):
            lanes = pl.ds(t * 128, 128)
            for p in range(2):
                ilv[ch][0, t, pl.ds(p, 32, stride=2), :] = value[p * 32 : p * 32 + 32, t * 128 : t * 128 + 128]
        C[ch, 2].wait_recv()
        C[ch, 5].wait_recv()
        value = cp[ch][0, 1] + rsin[ch][2] + rsfin[ch][1]
        for t in range(CHUNKS[ch] // 128):
            for p in range(2):
                ilv[ch][1, t, pl.ds(p, 32, stride=2), :] = value[p * 32 : p * 32 + 32, t * 128 : t * 128 + 128]
        for t in range(CHUNKS[ch] // 128):
            fin_s[ch][:, pl.ds(t * 128, 128)] = ilv[ch][1 - l, t].astype(BF16)
        c_copy(ch, 6, fin_s[ch], fin_r[ch], part)
        for t in range(CHUNKS[ch] // 128):
            col = l * HALF + (sum(CHUNKS[:ch]) + t * 128)
            out_ref[:, pl.ds(pl.multiple_of(col, 128), 128)] = ilv[ch][l, t].astype(BF16)

    def c_last(ch):
        C[ch, 6].wait_recv()
        out_ref[:, columns(ch, 1 - l)] = fin_r[ch][...]

    prep_own(0)
    b_own(0)
    prep_other(0)
    b_pair(0)
    ax.wait_recv()
    a_prep(0)
    b_own_sib(0)
    a_prep(1)
    prep_other(1)
    b_pair(1)
    a_rest(0)
    a_prep(2)
    prep_own(1)
    b_other(0)
    b_own(1)
    b_own_sib(1)
    a_rest(1)
    a_forward(0)
    prep_other(2)
    b_pair(2)
    b_mid(0)
    b_other(1)
    prep_own(2)
    b_own(2)
    b_own_sib(2)
    a_rest(2)
    prep_other(3)
    b_pair(3)
    prep_own(3)
    a_forward(1)
    b_far(0)
    b_mid(1)
    a_forward(2)
    b_other(2)
    b_own(3)
    b_own_sib(3)
    a_ready(0)
    b_ready(0)
    c_far(0)
    b_far(1)
    a_ready(1)
    c_near(0)
    b_mid(2)
    b_other(3)
    c_combine(0)
    b_ready(1)
    c_far(1)
    c_near(1)
    a_ready(2)
    c_own(0)
    c_final(0)
    b_far(2)
    b_mid(3)
    c_combine(1)
    b_ready(2)
    c_far(2)
    c_near(2)
    c_own(1)
    c_final(1)
    b_far(3)
    c_last(0)
    c_combine(2)
    b_ready(3)
    c_far(3)
    c_near(3)
    c_own(2)
    c_final(2)
    c_last(1)
    c_own(3)
    c_combine(3)
    c_last(2)
    c_final(3)
    c_last(3)
    for copy in pending:
        copy.wait_send()


def body(a_blocks, a_mask, a_row_ids, a_col_ids, b_matrix, b_mask):
    blocks = a_blocks.reshape(32, 2, 32, 128).transpose(0, 2, 1, 3).reshape(32, 64, 128)
    order = jnp.arange(64, dtype=jnp.int32)
    slots = jnp.sum(jnp.where(a_row_ids[None, :] == order[:, None], order[None, :], 0), axis=1)
    vmem = pl.BlockSpec(memory_space=pltpu.VMEM)
    smem = pl.BlockSpec(memory_space=pltpu.SMEM)
    n, groups = len(CHUNKS), len(GROUPS)
    rows = [128 * len(group) for group in GROUPS]
    dma = pltpu.SemaphoreType.DMA
    scratch = [
        pltpu.VMEM((64, 64, 128), BF16),
        pltpu.VMEM((8, 64, 128), F32),
        [pltpu.VMEM((2, 64, w), BF16) for w in CHUNKS],
        [pltpu.VMEM((3, m, 128), BF16) for m in rows],
        [pltpu.VMEM((16, m, 128), BF16) for m in rows],
        [pltpu.VMEM((8, 4, 64, w), BF16) for w in CHUNKS],
        [pltpu.VMEM((2048, w), BF16) for w in CHUNKS],
        [pltpu.VMEM((4, 2, 64, w), F32) for w in CHUNKS],
        [pltpu.VMEM((4, 64, w), F32) for w in CHUNKS],
        [pltpu.VMEM((2, 64, w), F32) for w in CHUNKS],
        [pltpu.VMEM((2, 64, w), F32) for w in CHUNKS],
        [pltpu.VMEM((2, w // 128, 64, 128), F32) for w in CHUNKS],
        [pltpu.VMEM((64, w), BF16) for w in CHUNKS],
        [pltpu.VMEM((64, w), BF16) for w in CHUNKS],
        dma, dma,
        dma((groups, 15)), dma((groups, 15)),
        dma((n, 15)), dma((n, 15)),
        dma((n, 7)), dma((n, 7)),
    ]
    return pl.pallas_call(
        kernel,
        out_shape=jax.ShapeDtypeStruct((64, 3072), BF16),
        in_specs=[smem, smem, smem, smem, vmem, vmem],
        out_specs=vmem,
        scratch_shapes=scratch,
        compiler_params=pltpu.CompilerParams(collective_id=0, has_side_effects=True),
        name="contract",
    )(slots, a_col_ids, a_mask.T, b_mask, blocks, b_matrix)


def solution(mesh):
    return jax.shard_map(
        body,
        mesh=mesh,
        in_specs=(
            P("row", ("col", "depth"), None),
            P("row", ("col", "depth")),
            P(),
            P(),
            P(("row", "depth"), "col"),
            P(("row", "depth"), "col"),
        ),
        out_specs=P(("row", "depth"), "col"),
        check_vma=False,
    )
```

```python
import jax
import jax.numpy as jnp
from jax import lax
from jax.experimental import pallas as pl
from jax.experimental.pallas import tpu as pltpu
from jax.sharding import PartitionSpec as P

MESH = pl.DeviceIdType.MESH
CHUNKS = (256, 256, 256, 256, 256, 128, 128)
GROUPS = (((2, 0), (2, 1)), ((1, 1), (3, 0)), ((1, 0), (3, 1)), ((0, 0), (0, 1)))
BY_OTHER = (0, 1, 3)
A_DIRECT = ()
B_DIRECT = ()
LAST_DIRECT = (5, 6)
HALF = 1536
F32 = jnp.float32
BF16 = jnp.bfloat16

AX, B_PAIR, B_OWN, B_OTHER, B_MID, B_SIDE, B_FAR, B_READY, A_PREP, A_RING, A_FWD, A_READY = range(12)
C_FAR, C_NEAR, C_PRE, C_COMB, C_OWN, C_FINAL, C_LAST = range(12, 19)

ORDER = (
    (B_OWN, 3), (B_PAIR, 0), (AX,), (B_OWN, 0), (B_PAIR, 3), (A_PREP, 0, 2), (A_PREP, 0, 1), (A_PREP, 0, 3),
    (B_PAIR, 1), (A_PREP, 0, 0), (A_PREP, 1, 2), (A_PREP, 1, 1), (B_PAIR, 4), (A_PREP, 1, 3), (A_PREP, 2, 2),
    (B_MID, 3, 0), (A_PREP, 1, 0), (B_OTHER, 3), (A_RING, 0, 1), (B_OWN, 1), (A_RING, 0, 3), (A_RING, 0, 2),
    (B_OTHER, 1), (A_RING, 1, 2), (A_PREP, 2, 1), (A_RING, 1, 3), (A_RING, 1, 1), (B_MID, 3, 1), (A_FWD, 0, 1),
    (B_PAIR, 2), (A_FWD, 1, 0), (A_FWD, 0, 2), (A_PREP, 2, 3), (B_OTHER, 0), (A_FWD, 0, 0), (B_MID, 1, 1),
    (A_FWD, 0, 3), (B_MID, 1, 0), (A_FWD, 1, 3), (A_FWD, 1, 2), (A_PREP, 3, 2), (A_FWD, 1, 1), (A_PREP, 3, 1),
    (A_PREP, 2, 0), (A_PREP, 3, 3), (A_RING, 2, 2), (B_FAR, 3), (B_SIDE, 3), (A_RING, 2, 1), (B_SIDE, 1),
    (B_READY, 3), (A_RING, 2, 3), (B_PAIR, 5), (B_MID, 0, 0), (A_READY, 0), (B_MID, 0, 1), (B_OWN, 2), (C_FAR, 3),
    (A_FWD, 2, 0), (A_READY, 1), (B_FAR, 1), (B_PAIR, 6), (C_NEAR, 3), (A_FWD, 2, 1), (B_SIDE, 0), (A_FWD, 2, 2),
    (B_OTHER, 2), (B_READY, 1), (C_FAR, 1), (A_FWD, 2, 3), (C_NEAR, 1), (B_OWN, 4), (B_OTHER, 4), (A_RING, 3, 3),
    (A_PREP, 3, 0), (A_RING, 3, 2), (B_FAR, 0), (B_MID, 2, 0), (B_READY, 0), (C_FAR, 0), (C_NEAR, 0), (A_RING, 3, 1),
    (A_READY, 2), (C_PRE, 3), (C_PRE, 1), (B_MID, 2, 1), (C_COMB, 3, 0), (B_OTHER, 6), (C_COMB, 3, 1), (C_COMB, 1, 1),
    (B_OWN, 6), (A_FWD, 3, 3), (B_SIDE, 2), (A_FWD, 3, 0), (C_COMB, 1, 0), (C_PRE, 0), (A_FWD, 3, 1), (A_FWD, 3, 2),
    (B_MID, 4, 1), (B_MID, 4, 0), (C_COMB, 0, 1), (C_COMB, 0, 0), (B_FAR, 2), (B_OWN, 5), (B_OTHER, 5), (B_SIDE, 4),
    (B_READY, 2), (B_MID, 6, 0), (C_FAR, 2), (B_MID, 6, 1), (A_READY, 3), (C_OWN, 3), (B_SIDE, 6), (C_FINAL, 3),
    (C_OWN, 1), (B_FAR, 4), (C_OWN, 0), (C_NEAR, 2), (C_PRE, 2), (C_FINAL, 1), (B_MID, 5, 0), (B_MID, 5, 1),
    (B_READY, 4), (C_FAR, 4), (C_FINAL, 0), (B_FAR, 6), (C_COMB, 2, 1), (C_COMB, 2, 0), (B_SIDE, 5), (C_OWN, 2),
    (B_READY, 6), (C_OWN, 6), (C_PRE, 4), (C_FAR, 6), (C_PRE, 6), (B_FAR, 5), (C_NEAR, 4), (B_READY, 5), (C_FAR, 5),
    (C_COMB, 4, 0), (C_COMB, 4, 1), (C_OWN, 5), (C_OWN, 4), (C_FINAL, 2), (C_LAST, 1), (C_COMB, 6, 0), (C_COMB, 6, 1),
    (C_LAST, 3), (C_NEAR, 5), (C_PRE, 5), (C_COMB, 5, 1), (C_LAST, 0), (C_NEAR, 6), (C_COMB, 5, 0), (C_LAST, 2),
    (C_FINAL, 4), (C_FINAL, 5), (C_LAST, 4), (C_FINAL, 6),
)


def kernel(
    rowid_hbm, colid_hbm, amask_hbm, bmask_hbm, a_hbm, b_hbm, out_ref,
    rowid_ref, colid_ref, amask_ref, bmask_ref, a_ref, b_ref, in_sem, slotv, slot_ref, araw, tmp, bxs, pst, abuf, bbuf, rbuf, cp, rsin, rsout, rsfin, ilv, fin_s, fin_r, last,
    slot_sem, sx_s, sx_r, sa_s, sa_r, sb_s, sb_r, sc_s, sc_r, sf_s,
):
    r = lax.axis_index("row")
    c = lax.axis_index("col")
    d = lax.axis_index("depth")
    z = lax.div(d, 8)
    y = lax.rem(lax.div(d, 2), 4)
    l = lax.rem(d, 2)
    x = c * 2 + l
    x_part = c * 2 + (1 - l)
    x_other = lax.rem(x + 3 + 2 * l, 4)
    x_far = lax.rem(x + 2, 4)

    def dev(xx, yy, zz):
        return (r, lax.div(xx, 2), zz * 8 + yy * 2 + lax.rem(xx, 2))

    def dev_y(k):
        return dev(x, lax.rem(y + k, 4), z)

    def dev_z(k):
        return dev(x, y, lax.rem(z + k, 4))

    part, other, far = dev(x_part, y, z), dev(x_other, y, z), dev(x_far, y, z)
    sib = (1 - r, c, d)
    def rcopy(src, dst, ss, rs, target):
        copy = pltpu.make_async_remote_copy(
            src_ref=src, dst_ref=dst, send_sem=ss, recv_sem=rs, device_id=target, device_id_type=MESH
        )
        copy.start()
        return copy

    def bytes_of(ref, ss, rs):
        return pltpu.make_async_remote_copy(
            src_ref=ref, dst_ref=ref, send_sem=ss, recv_sem=rs, device_id=sib, device_id_type=MESH
        )

    barrier = pltpu.get_barrier_semaphore()
    peers = [dev_y(1), dev_y(2), dev_y(3), dev_z(1), dev_z(3), part, other, sib] + ([far] if A_DIRECT else [])
    if LAST_DIRECT:
        peers += [dev(x_part, y, lax.rem(z + 1, 4)), dev(x_part, y, lax.rem(z + 3, 4))]
    for peer in peers:
        pl.semaphore_signal(barrier, inc=1, device_id=peer, device_id_type=MESH)

    inputs = ((rowid_hbm, rowid_ref), (amask_hbm, amask_ref), (a_hbm, a_ref), (bmask_hbm, bmask_ref), (b_hbm, b_ref), (colid_hbm, colid_ref))
    loads = [pltpu.make_async_copy(src, dst, in_sem.at[i]) for i, (src, dst) in enumerate(inputs)]
    for load in loads:
        load.start()

    loads[0].wait()
    place = lax.broadcasted_iota(jnp.int32, (8, 128), 1)
    slots = jnp.zeros((8, 128), jnp.int32)
    for u in range(64):
        slots = jnp.where(place == rowid_ref[u], u, slots)
    slotv[...] = slots

    odd = lax.rem(lax.broadcasted_iota(jnp.int32, (64, 128), 0), 2) == 1

    def mask_a(u, _):
        factor = jnp.where(odd, amask_ref[1, u], amask_ref[0, u]).astype(F32)
        araw[r * 32 + u] = (a_ref[u].astype(F32) * factor).astype(BF16)
        return 0

    loads[1].wait()
    loads[2].wait()
    lax.fori_loop(0, 32, mask_a, 0, unroll=4)
    to_smem = pltpu.make_async_copy(slotv, slot_ref, slot_sem)
    to_smem.start()

    for load in loads[3:]:
        load.wait()
    pl.semaphore_wait(barrier, len(peers))
    left_lane = lax.broadcasted_iota(jnp.int32, (64, 128), 1) < 64
    own_plane = y * 2 + l
    two = pl.ds(r * 2, 2)
    exchange = []

    def ax():
        mine = pl.ds(r * 32, 32)
        exchange.append(rcopy(araw.at[mine], araw.at[mine], sx_s, sx_r, sib))
        to_smem.wait()

    def mask_b(ch, half):
        start = sum(CHUNKS[:ch])
        for j in range(2):
            for t in range(CHUNKS[ch] // 128):
                col = half * HALF + (start + t * 128)
                block = half * (HALF // 64) + (start // 64 + t * 2)
                factor = jnp.where(left_lane, bmask_ref[j, block], bmask_ref[j, block + 1]).astype(F32)
                tile = b_ref[pl.ds(j * 64, 64), pl.ds(pl.multiple_of(col, 128), 128)].astype(F32)
                yield j, t, (tile * factor).astype(BF16)

    def piece(ch, k, lam):
        plane = lax.rem(y + k, 4) * 2 + (l if lam == 0 else 1 - l)
        return bbuf[ch].at[plane, two]

    def b_copy(ch, i, ref, target):
        rcopy(ref, ref, sb_s.at[ch], sb_r.at[ch, i], target)

    def b_wait(ch, i, pieces):
        bytes_of(rbuf[ch].at[pl.ds(0, 128 * pieces)], sb_s.at[ch], sb_r.at[ch, i]).wait_recv()

    def b_pair(ch):
        for j, t, tile in mask_b(ch, 1 - l):
            bxs[ch][j, :, pl.ds(t * 128, 128)] = tile
        rcopy(bxs[ch], bbuf[ch].at[own_plane, two], sb_s.at[ch], sb_r.at[ch, 0], part)

    def b_own(ch):
        for j, t, tile in mask_b(ch, l):
            bbuf[ch][own_plane, r * 2 + j, :, pl.ds(t * 128, 128)] = tile
        b_copy(ch, 1, piece(ch, 0, 0), dev_y(1))
        b_copy(ch, 3, piece(ch, 0, 0), dev_y(3))
        if ch in B_DIRECT:
            b_copy(ch, 4, piece(ch, 0, 0), dev_y(2))
        b_copy(ch, 5, piece(ch, 0, 0), sib)

    def b_other(ch):
        b_wait(ch, 0, 1)
        b_copy(ch, 3, piece(ch, 0, 1), dev_y(1))
        b_copy(ch, 2, piece(ch, 0, 1), dev_y(3))
        if ch in B_DIRECT:
            b_copy(ch, 4, piece(ch, 0, 1), dev_y(2))
        b_copy(ch, 5, piece(ch, 0, 1), sib)

    def b_mid(ch, lam):
        b_wait(ch, 1 + lam, 1)
        ref = piece(ch, 3 - 2 * lam, lam)
        if ch not in B_DIRECT:
            b_copy(ch, 4, ref, dev_y(1 + 2 * lam))
        b_copy(ch, 5, ref, sib)

    def b_side(ch):
        b_wait(ch, 3, 2)
        b_copy(ch, 5, piece(ch, 1, 0), sib)
        b_copy(ch, 5, piece(ch, 3, 1), sib)

    def b_far(ch):
        b_wait(ch, 4, 2)
        b_copy(ch, 5, piece(ch, 2, 0), sib)
        b_copy(ch, 5, piece(ch, 2, 1), sib)

    def b_ready(ch):
        b_wait(ch, 5, 8)
        for plane in range(8):
            for cc in range(2):
                for jj in range(2):
                    k = colid_ref[(cc * 32 + z * 8 + plane) * 2 + jj]
                    sel = lax.div(k, 64) * 2 + lax.rem(k, 2)
                    rbuf[ch][pl.ds((plane * 4 + cc * 2 + jj) * 64, 64), :] = bbuf[ch][plane, sel]

    def source(xx, yy):
        return (yy * 2 + lax.rem(xx, 2)) * 2 + lax.div(xx, 2)

    def held(g, xx, k):
        return abuf[g].at[source(xx, lax.rem(y + 4 - k, 4))]

    def a_copy(g, i, src, dst, target):
        rcopy(src, dst, sa_s.at[g], sa_r.at[g, i], target)

    def a_wait(g, i, pieces):
        bytes_of(abuf[g].at[pl.ds(0, pieces)], sa_s.at[g], sa_r.at[g, i]).wait_recv()

    def a_prep(g, k):
        if (g, k) == (0, 2):
            exchange[0].wait_recv()
        yy = lax.rem(y + k, 4)
        for n, (zr, ll) in enumerate(GROUPS[g]):
            zz = lax.rem(z + zr, 4)
            u = slot_ref[0, r * 32 + zz * 8 + yy * 2 + ll]
            slot = (k * 2 + n) % 8
            tmp[slot] = araw[u].astype(F32)
            first = tmp[slot, pl.ds(0, 32, stride=2), :]
            second = tmp[slot, pl.ds(1, 32, stride=2), :]
            lane = left_lane[:32]
            even = jnp.where(lane, first, pltpu.roll(second, 64, 1))
            oddr = jnp.where(lane, pltpu.roll(first, 64, 1), second)
            block = jnp.concatenate([even, oddr], axis=0).astype(BF16)
            if k == 0:
                abuf[g][source(x, y), pl.ds(n * 64, 64), :] = block
            else:
                pst[g][k - 1, pl.ds(n * 64, 64), :] = block
        if k:
            a_copy(g, k - 1, pst[g].at[k - 1], abuf[g].at[source(x, y)], dev_y(k))
        else:
            a_send(g, 0)

    def a_send(g, k):
        ref = held(g, x, k)
        onward = g not in A_DIRECT
        a_copy(g, 3 + k if onward and k in BY_OTHER else 7, ref, ref, part)
        a_copy(g, 3 + k if onward and k not in BY_OTHER else 7, ref, ref, other)
        if not onward:
            a_copy(g, 7, ref, ref, far)

    def a_ring(g, k):
        a_wait(g, k - 1, 1)
        a_send(g, k)

    def a_fwd(g, k):
        a_wait(g, 3 + k, 1)
        via, target = (x_part, other) if k in BY_OTHER else (x_other, part)
        ref = held(g, via, k)
        a_copy(g, 7, ref, ref, target)

    def a_ready(g):
        a_wait(g, 7, 12 if g in A_DIRECT else 8)

    def multiply(ch, g):
        lhs = jnp.concatenate([abuf[g][i] for i in range(16)], axis=1)
        total = jnp.dot(lhs, rbuf[ch][...], preferred_element_type=F32)
        for n, unit in enumerate(GROUPS[g]):
            cp[ch][unit] = total[n * 64 : n * 64 + 64]

    def c_copy(ch, i, src, dst, target):
        rcopy(src, dst, sc_s.at[ch], sc_r.at[ch, i], target)

    def c_wait(ch, i, ref):
        bytes_of(ref, sc_s.at[ch], sc_r.at[ch, i]).wait_recv()

    def last_copy(ch, src, kind, target):
        rcopy(src, last[LAST_DIRECT.index(ch)].at[kind, l], sc_s.at[ch], sc_r.at[ch, 2], target)

    def c_far(ch):
        multiply(ch, 0)
        c_copy(ch, 0, cp[ch].at[2, 0], rsin[ch].at[0], dev_z(1))
        c_copy(ch, 1, cp[ch].at[2, 1], rsin[ch].at[1], dev_z(3))

    def c_near(ch):
        multiply(ch, 1)
        if ch in LAST_DIRECT:
            last_copy(ch, cp[ch].at[1, 1], 0, dev(c * 2 + 1, y, lax.rem(z + 1, 4)))
            last_copy(ch, cp[ch].at[3, 0], 0, dev(c * 2, y, lax.rem(z + 3, 4)))
        else:
            c_copy(ch, 2, cp[ch].at[1, 1], rsin[ch].at[2], dev_z(1))
            c_copy(ch, 2, cp[ch].at[3, 0], rsin[ch].at[3], dev_z(3))

    def c_pre(ch):
        multiply(ch, 2)

    def c_comb(ch, n):
        c_wait(ch, n, cp[ch].at[0, 0])
        rsout[ch][n] = rsin[ch][n] + cp[ch][1 + 2 * n, n]
        if ch in LAST_DIRECT:
            last_copy(ch, rsout[ch].at[n], 1, dev(c * 2 + n, y, lax.rem(z + 1 + 2 * n, 4)))
            return
        c_copy(ch, 2, rsout[ch].at[n], rsfin[ch].at[n], dev_z(1 + 2 * n))

    def c_own(ch):
        multiply(ch, 3)
        if ch in LAST_DIRECT:
            rcopy(cp[ch].at[0, 1 - l], last[LAST_DIRECT.index(ch)].at[2, l], sf_s.at[1 + LAST_DIRECT.index(ch)], sc_r.at[ch, 3], part)

    def out_half(ch, s, h):
        for t in range(CHUNKS[ch] // 128):
            col = s * HALF + (sum(CHUNKS[:ch]) + t * 128)
            out_ref[:, pl.ds(pl.multiple_of(col, 128), 128)] = ilv[ch][h, t].astype(BF16)

    def interleave(ch, h, value):
        for t in range(CHUNKS[ch] // 128):
            for p in range(2):
                half = value[p * 32 : p * 32 + 32, t * 128 : t * 128 + 128]
                ilv[ch][h, t, pl.ds(p, 32, stride=2), :] = half

    def c_final_direct(ch):
        at = LAST_DIRECT.index(ch)
        c_wait(ch, 2, cp[ch].at[pl.ds(0, 2)])
        c_wait(ch, 3, cp[ch].at[0, 0])
        for n, s in enumerate((l, 1 - l)):
            own = last[at][2, s] if n else cp[ch][0, l]
            interleave(ch, n, own + last[at][0, s] + last[at][1, s])
            out_half(ch, s, n)

    def c_final(ch):
        if ch in LAST_DIRECT:
            return c_final_direct(ch)
        c_wait(ch, 2, cp[ch].at[pl.ds(0, 2)])
        for h in range(2):
            value = cp[ch][0, h] + rsin[ch][3 - h] + rsfin[ch][h]
            interleave(ch, h, value)
        for t in range(CHUNKS[ch] // 128):
            fin_s[ch][:, pl.ds(t * 128, 128)] = ilv[ch][1 - l, t].astype(BF16)
        rcopy(fin_s[ch], fin_r[ch], sf_s.at[0], sc_r.at[ch, 3], part)
        out_half(ch, l, l)

    def c_last(ch):
        c_wait(ch, 3, fin_r[ch])
        col = (1 - l) * HALF + sum(CHUNKS[:ch])
        out_ref[:, pl.ds(pl.multiple_of(col, 128), CHUNKS[ch])] = fin_r[ch][...]

    steps = (
        ax, b_pair, b_own, b_other, b_mid, b_side, b_far, b_ready, a_prep, a_ring, a_fwd, a_ready,
        c_far, c_near, c_pre, c_comb, c_own, c_final, c_last,
    )
    for step, *where in ORDER:
        steps[step](*where)

    exchange[0].wait_send()
    for g in range(len(GROUPS)):
        bytes_of(abuf[g].at[pl.ds(0, 15)], sa_s.at[g], sa_r.at[g, 0]).wait_send()
    for ch in range(len(CHUNKS)):
        bytes_of(rbuf[ch].at[pl.ds(0, 1920)], sb_s.at[ch], sb_r.at[ch, 0]).wait_send()
        bytes_of(cp[ch].at[pl.ds(0, 3)], sc_s.at[ch], sc_r.at[ch, 0]).wait_send()
    for at, ch in enumerate(LAST_DIRECT):
        bytes_of(cp[ch].at[0, 0], sf_s.at[1 + at], sc_r.at[ch, 3]).wait_send()
    width = sum(CHUNKS[ch] for ch in range(len(CHUNKS)) if ch not in LAST_DIRECT)
    bytes_of(b_ref.at[pl.ds(0, 64), pl.ds(0, width)], sf_s.at[0], sc_r.at[0, 3]).wait_send()


def body(a_blocks, a_mask, a_row_ids, a_col_ids, b_matrix, b_mask):
    blocks = a_blocks.reshape(32, 2, 32, 128).transpose(0, 2, 1, 3).reshape(32, 64, 128)
    vmem = pl.BlockSpec(memory_space=pltpu.VMEM)
    hbm = pl.BlockSpec(memory_space=pltpu.HBM)
    n, groups = len(CHUNKS), len(GROUPS)
    rows = [128] * groups
    dma = pltpu.SemaphoreType.DMA
    scratch = [
        pltpu.SMEM((64,), jnp.int32),
        pltpu.SMEM((128,), jnp.int32),
        pltpu.SMEM((2, 32), jnp.int32),
        pltpu.SMEM((2, 48), jnp.int32),
        pltpu.VMEM((32, 64, 128), BF16),
        pltpu.VMEM((128, 3072), BF16),
        dma((6,)),
        pltpu.VMEM((8, 128), jnp.int32),
        pltpu.SMEM((8, 128), jnp.int32),
        pltpu.VMEM((64, 64, 128), BF16),
        pltpu.VMEM((8, 64, 128), F32),
        [pltpu.VMEM((2, 64, w), BF16) for w in CHUNKS],
        [pltpu.VMEM((3, m, 128), BF16) for m in rows],
        [pltpu.VMEM((16, m, 128), BF16) for m in rows],
        [pltpu.VMEM((8, 4, 64, w), BF16) for w in CHUNKS],
        [pltpu.VMEM((2048, w), BF16) for w in CHUNKS],
        [pltpu.VMEM((4, 2, 64, w), F32) for w in CHUNKS],
        [pltpu.VMEM((4, 64, w), F32) for w in CHUNKS],
        [pltpu.VMEM((2, 64, w), F32) for w in CHUNKS],
        [pltpu.VMEM((2, 64, w), F32) for w in CHUNKS],
        [pltpu.VMEM((2, w // 128, 64, 128), F32) for w in CHUNKS],
        [pltpu.VMEM((64, w), BF16) for w in CHUNKS],
        [pltpu.VMEM((64, w), BF16) for w in CHUNKS],
        [pltpu.VMEM((3, 2, 64, CHUNKS[ch]), F32) for ch in LAST_DIRECT],
        dma, dma, dma,
        dma((groups,)), dma((groups, 8)),
        dma((n,)), dma((n, 6)),
        dma((n,)), dma((n, 4)),
        dma((1 + len(LAST_DIRECT),)),
    ]
    return pl.pallas_call(
        kernel,
        out_shape=pltpu.VMEM((64, 3072), BF16),
        in_specs=[hbm] * 6,
        out_specs=vmem,
        scratch_shapes=scratch,
        compiler_params=pltpu.CompilerParams(collective_id=0, has_side_effects=True),
        name="contract",
    )(a_row_ids, a_col_ids, a_mask.T, b_mask, blocks, b_matrix)


def solution(mesh):
    return jax.shard_map(
        body,
        mesh=mesh,
        in_specs=(
            P("row", ("col", "depth"), None),
            P("row", ("col", "depth")),
            P(),
            P(),
            P(("row", "depth"), "col"),
            P(("row", "depth"), "col"),
        ),
        out_specs=P(("row", "depth"), "col"),
        check_vma=False,
    )
```

```python
import jax
import jax.numpy as jnp
from jax import lax
from jax.experimental import pallas as pl
from jax.experimental.pallas import tpu as pltpu
from jax.sharding import PartitionSpec as P

MESH = pl.DeviceIdType.MESH
CHUNKS = (256, 256, 256, 256, 256, 128, 128)
GROUPS = (((2, 0), (2, 1)), ((1, 1), (3, 0)), ((1, 0), (3, 1)), ((0, 0), (0, 1)))
BY_OTHER = (0, 1, 3)
A_DIRECT = ()
B_DIRECT = ()
LAST_DIRECT = (5, 6)
ALL_DIRECT = ()
HALF = 1536
F32 = jnp.float32
BF16 = jnp.bfloat16

AX, B_PAIR, B_OWN, B_OTHER, B_MID, B_SIDE, B_FAR, B_READY, A_PREP, A_RING, A_FWD, A_READY = range(12)
C_FAR, C_NEAR, C_PRE, C_COMB, C_OWN, C_FINAL, C_LAST = range(12, 19)

ORDER = (
    (B_OWN, 3), (B_PAIR, 3), (AX,), (B_PAIR, 1), (B_OWN, 0), (A_PREP, 0, 2), (A_PREP, 0, 1), (A_PREP, 0, 3),
    (A_PREP, 0, 0), (A_PREP, 1, 2), (A_PREP, 1, 1), (A_PREP, 1, 3), (B_PAIR, 0), (B_OTHER, 3), (B_PAIR, 2),
    (B_OWN, 1), (A_PREP, 1, 0), (A_RING, 0, 1), (A_RING, 0, 2), (B_OTHER, 1), (A_RING, 0, 3), (A_PREP, 2, 2),
    (A_RING, 1, 3), (A_RING, 1, 1), (B_MID, 3, 0), (A_RING, 1, 2), (B_PAIR, 4), (A_FWD, 0, 0), (B_MID, 3, 1),
    (A_PREP, 2, 1), (B_MID, 1, 0), (A_FWD, 0, 1), (B_OTHER, 0), (A_FWD, 0, 3), (A_FWD, 0, 2), (A_FWD, 1, 0),
    (A_PREP, 2, 3), (B_MID, 1, 1), (B_SIDE, 3), (A_FWD, 1, 3), (A_FWD, 1, 1), (A_PREP, 2, 0), (A_PREP, 3, 2),
    (A_FWD, 1, 2), (B_MID, 0, 0), (A_PREP, 3, 1), (A_PREP, 3, 3), (B_SIDE, 1), (B_FAR, 3), (A_RING, 2, 2),
    (A_RING, 2, 1), (B_MID, 0, 1), (A_READY, 0), (A_RING, 2, 3), (B_OWN, 2), (B_READY, 3), (C_FAR, 3), (A_PREP, 3, 0),
    (B_FAR, 1), (B_SIDE, 0), (A_READY, 1), (B_OTHER, 2), (B_OWN, 4), (C_NEAR, 3), (B_PAIR, 6), (A_FWD, 2, 0),
    (A_FWD, 2, 2), (A_FWD, 2, 1), (B_READY, 1), (C_FAR, 1), (A_FWD, 2, 3), (B_FAR, 0), (C_NEAR, 1), (A_RING, 3, 2),
    (A_RING, 3, 3), (B_OTHER, 4), (A_FWD, 3, 0), (A_RING, 3, 1), (B_PAIR, 5), (B_READY, 0), (C_FAR, 0), (B_MID, 2, 0),
    (C_NEAR, 0), (B_MID, 2, 1), (A_READY, 2), (C_PRE, 3), (C_PRE, 1), (C_COMB, 3, 1), (C_COMB, 1, 1), (B_OWN, 6),
    (C_COMB, 3, 0), (B_MID, 4, 0), (A_FWD, 3, 2), (C_COMB, 1, 0), (B_OTHER, 6), (C_PRE, 0), (B_SIDE, 2),
    (A_FWD, 3, 3), (B_MID, 4, 1), (B_OTHER, 5), (A_FWD, 3, 1), (B_OWN, 5), (C_COMB, 0, 1), (B_SIDE, 4),
    (C_COMB, 0, 0), (B_FAR, 2), (B_MID, 6, 0), (B_MID, 6, 1), (B_READY, 2), (C_FAR, 2), (A_READY, 3), (C_OWN, 3),
    (C_OWN, 2), (C_FINAL, 3), (B_FAR, 4), (C_OWN, 1), (C_NEAR, 2), (B_MID, 5, 1), (C_OWN, 0), (C_FINAL, 1),
    (B_MID, 5, 0), (B_READY, 4), (C_FAR, 4), (B_SIDE, 6), (C_FINAL, 0), (B_FAR, 6), (B_SIDE, 5), (C_PRE, 2),
    (C_PRE, 4), (C_COMB, 2, 1), (C_COMB, 2, 0), (B_READY, 6), (C_FAR, 6), (B_FAR, 5), (C_NEAR, 4), (C_LAST, 0),
    (C_OWN, 6), (B_READY, 5), (C_FAR, 5), (C_COMB, 4, 1), (C_COMB, 4, 0), (C_PRE, 6), (C_OWN, 5), (C_FINAL, 2),
    (C_COMB, 6, 0), (C_COMB, 6, 1), (C_NEAR, 6), (C_NEAR, 5), (C_PRE, 5), (C_COMB, 5, 1), (C_OWN, 4), (C_COMB, 5, 0),
    (C_LAST, 3), (C_FINAL, 4), (C_LAST, 1), (C_FINAL, 6), (C_LAST, 2), (C_LAST, 4), (C_FINAL, 5),
)


def kernel(
    rowid_hbm, colid_hbm, amask_hbm, bmask_hbm, a_hbm, b_hbm, out_ref,
    rowid_ref, colid_ref, amask_ref, bmask_ref, a_ref, b_ref, in_sem, slotv, slot_ref, araw, tmp, bxs, pst, abuf, bbuf, rbuf, cp, rsin, rsout, rsfin, ilv, fin_s, fin_r, last,
    slot_sem, sx_s, sx_r, sa_s, sa_r, sb_s, sb_r, sc_s, sc_r, sf_s,
):
    r = lax.axis_index("row")
    c = lax.axis_index("col")
    d = lax.axis_index("depth")
    z = lax.div(d, 8)
    y = lax.rem(lax.div(d, 2), 4)
    l = lax.rem(d, 2)
    x = c * 2 + l
    x_part = c * 2 + (1 - l)
    x_other = lax.rem(x + 3 + 2 * l, 4)
    x_far = lax.rem(x + 2, 4)

    def dev(xx, yy, zz):
        return (r, lax.div(xx, 2), zz * 8 + yy * 2 + lax.rem(xx, 2))

    def dev_y(k):
        return dev(x, lax.rem(y + k, 4), z)

    def dev_z(k):
        return dev(x, y, lax.rem(z + k, 4))

    part, other, far = dev(x_part, y, z), dev(x_other, y, z), dev(x_far, y, z)
    sib = (1 - r, c, d)
    def rcopy(src, dst, ss, rs, target):
        copy = pltpu.make_async_remote_copy(
            src_ref=src, dst_ref=dst, send_sem=ss, recv_sem=rs, device_id=target, device_id_type=MESH
        )
        copy.start()
        return copy

    def bytes_of(ref, ss, rs):
        return pltpu.make_async_remote_copy(
            src_ref=ref, dst_ref=ref, send_sem=ss, recv_sem=rs, device_id=sib, device_id_type=MESH
        )

    barrier = pltpu.get_barrier_semaphore()
    peers = [dev_y(1), dev_y(2), dev_y(3), dev_z(1), dev_z(3), part, other, sib] + ([far] if A_DIRECT else [])
    if LAST_DIRECT:
        peers += [dev(x_part, y, lax.rem(z + 1, 4)), dev(x_part, y, lax.rem(z + 3, 4))]
    if ALL_DIRECT:
        peers += [dev_z(2), dev(x_part, y, lax.rem(z + 2, 4))]
    for peer in peers:
        pl.semaphore_signal(barrier, inc=1, device_id=peer, device_id_type=MESH)

    inputs = ((rowid_hbm, rowid_ref), (amask_hbm, amask_ref), (a_hbm, a_ref), (bmask_hbm, bmask_ref), (b_hbm, b_ref), (colid_hbm, colid_ref))
    loads = [pltpu.make_async_copy(src, dst, in_sem.at[i]) for i, (src, dst) in enumerate(inputs)]
    for load in loads:
        load.start()

    loads[0].wait()
    place = lax.broadcasted_iota(jnp.int32, (8, 128), 1)
    slots = jnp.zeros((8, 128), jnp.int32)
    for u in range(64):
        slots = jnp.where(place == rowid_ref[u], u, slots)
    slotv[...] = slots

    odd = lax.rem(lax.broadcasted_iota(jnp.int32, (64, 128), 0), 2) == 1

    def mask_a(u, _):
        factor = jnp.where(odd, amask_ref[1, u], amask_ref[0, u]).astype(F32)
        araw[r * 32 + u] = (a_ref[u].astype(F32) * factor).astype(BF16)
        return 0

    loads[1].wait()
    loads[2].wait()
    lax.fori_loop(0, 32, mask_a, 0, unroll=4)
    to_smem = pltpu.make_async_copy(slotv, slot_ref, slot_sem)
    to_smem.start()

    left_lane = lax.broadcasted_iota(jnp.int32, (64, 128), 1) < 64
    own_plane = y * 2 + l
    two = pl.ds(r * 2, 2)

    def mask_b(ch, half):
        start = sum(CHUNKS[:ch])
        for j in range(2):
            for t in range(CHUNKS[ch] // 128):
                col = half * HALF + (start + t * 128)
                block = half * (HALF // 64) + (start // 64 + t * 2)
                factor = jnp.where(left_lane, bmask_ref[j, block], bmask_ref[j, block + 1]).astype(F32)
                tile = b_ref[pl.ds(j * 64, 64), pl.ds(pl.multiple_of(col, 128), 128)].astype(F32)
                yield j, t, (tile * factor).astype(BF16)

    def prep_pair(ch):
        for j, t, tile in mask_b(ch, 1 - l):
            bxs[ch][j, :, pl.ds(t * 128, 128)] = tile

    def prep_own(ch):
        for j, t, tile in mask_b(ch, l):
            bbuf[ch][own_plane, r * 2 + j, :, pl.ds(t * 128, 128)] = tile

    for load in loads[3:]:
        load.wait()
    early = ORDER[: ORDER.index((A_PREP, 0, 2))]
    for step, *where in early:
        if step == B_PAIR:
            prep_pair(*where)
        if step == B_OWN:
            prep_own(*where)
    pl.semaphore_wait(barrier, len(peers))
    exchange = []

    def ax():
        mine = pl.ds(r * 32, 32)
        exchange.append(rcopy(araw.at[mine], araw.at[mine], sx_s, sx_r, sib))
        to_smem.wait()

    def piece(ch, k, lam):
        plane = lax.rem(y + k, 4) * 2 + (l if lam == 0 else 1 - l)
        return bbuf[ch].at[plane, two]

    def b_copy(ch, i, ref, target):
        rcopy(ref, ref, sb_s.at[ch], sb_r.at[ch, i], target)

    def b_wait(ch, i, pieces):
        bytes_of(rbuf[ch].at[pl.ds(0, 128 * pieces)], sb_s.at[ch], sb_r.at[ch, i]).wait_recv()

    def b_pair(ch):
        if (B_PAIR, ch) not in early:
            prep_pair(ch)
        rcopy(bxs[ch], bbuf[ch].at[own_plane, two], sb_s.at[ch], sb_r.at[ch, 0], part)

    def b_own(ch):
        if (B_OWN, ch) not in early:
            prep_own(ch)
        b_copy(ch, 1, piece(ch, 0, 0), dev_y(1))
        b_copy(ch, 3, piece(ch, 0, 0), dev_y(3))
        if (ch, 0) in B_DIRECT:
            b_copy(ch, 4, piece(ch, 0, 0), dev_y(2))
        b_copy(ch, 5, piece(ch, 0, 0), sib)

    def b_other(ch):
        b_wait(ch, 0, 1)
        b_copy(ch, 3, piece(ch, 0, 1), dev_y(1))
        b_copy(ch, 2, piece(ch, 0, 1), dev_y(3))
        if (ch, 1) in B_DIRECT:
            b_copy(ch, 4, piece(ch, 0, 1), dev_y(2))
        b_copy(ch, 5, piece(ch, 0, 1), sib)

    def b_mid(ch, lam):
        b_wait(ch, 1 + lam, 1)
        ref = piece(ch, 3 - 2 * lam, lam)
        if (ch, lam) not in B_DIRECT:
            b_copy(ch, 4, ref, dev_y(1 + 2 * lam))
        b_copy(ch, 5, ref, sib)

    def b_side(ch):
        b_wait(ch, 3, 2)
        b_copy(ch, 5, piece(ch, 1, 0), sib)
        b_copy(ch, 5, piece(ch, 3, 1), sib)

    def b_far(ch):
        b_wait(ch, 4, 2)
        b_copy(ch, 5, piece(ch, 2, 0), sib)
        b_copy(ch, 5, piece(ch, 2, 1), sib)

    def b_ready(ch):
        b_wait(ch, 5, 8)
        for plane in range(8):
            for cc in range(2):
                for jj in range(2):
                    k = colid_ref[(cc * 32 + z * 8 + plane) * 2 + jj]
                    sel = lax.div(k, 64) * 2 + lax.rem(k, 2)
                    rbuf[ch][pl.ds((plane * 4 + cc * 2 + jj) * 64, 64), :] = bbuf[ch][plane, sel]

    def source(xx, yy):
        return (yy * 2 + lax.rem(xx, 2)) * 2 + lax.div(xx, 2)

    def held(g, xx, k):
        return abuf[g].at[source(xx, lax.rem(y + 4 - k, 4))]

    def a_copy(g, i, src, dst, target):
        rcopy(src, dst, sa_s.at[g], sa_r.at[g, i], target)

    def a_wait(g, i, pieces):
        bytes_of(abuf[g].at[pl.ds(0, pieces)], sa_s.at[g], sa_r.at[g, i]).wait_recv()

    def a_prep(g, k):
        if (g, k) == (0, 2):
            exchange[0].wait_recv()
        yy = lax.rem(y + k, 4)
        for n, (zr, ll) in enumerate(GROUPS[g]):
            zz = lax.rem(z + zr, 4)
            u = slot_ref[0, r * 32 + zz * 8 + yy * 2 + ll]
            slot = (k * 2 + n) % 8
            tmp[slot] = araw[u].astype(F32)
            first = tmp[slot, pl.ds(0, 32, stride=2), :]
            second = tmp[slot, pl.ds(1, 32, stride=2), :]
            lane = left_lane[:32]
            even = jnp.where(lane, first, pltpu.roll(second, 64, 1))
            oddr = jnp.where(lane, pltpu.roll(first, 64, 1), second)
            block = jnp.concatenate([even, oddr], axis=0).astype(BF16)
            if k == 0:
                abuf[g][source(x, y), pl.ds(n * 64, 64), :] = block
            else:
                pst[g][k - 1, pl.ds(n * 64, 64), :] = block
        if k:
            a_copy(g, k - 1, pst[g].at[k - 1], abuf[g].at[source(x, y)], dev_y(k))
        else:
            a_send(g, 0)

    def a_send(g, k):
        ref = held(g, x, k)
        onward = (g, k) not in A_DIRECT
        a_copy(g, 3 + k if onward and k in BY_OTHER else 7, ref, ref, part)
        a_copy(g, 3 + k if onward and k not in BY_OTHER else 7, ref, ref, other)
        if not onward:
            a_copy(g, 7, ref, ref, far)

    def a_ring(g, k):
        a_wait(g, k - 1, 1)
        a_send(g, k)

    def a_fwd(g, k):
        a_wait(g, 3 + k, 1)
        via, target = (x_part, other) if k in BY_OTHER else (x_other, part)
        ref = held(g, via, k)
        a_copy(g, 7, ref, ref, target)

    def a_ready(g):
        a_wait(g, 7, 8 + sum((g, k) in A_DIRECT for k in range(4)))

    def multiply(ch, g):
        total = None
        for k in range(0, 16, 4):
            lhs = jnp.concatenate([abuf[g][i] for i in range(k, k + 4)], axis=1)
            share = jnp.dot(lhs, rbuf[ch][pl.ds(k * 128, 512), :], preferred_element_type=F32)
            total = share if total is None else total + share
        for n, unit in enumerate(GROUPS[g]):
            cp[ch][unit] = total[n * 64 : n * 64 + 64]

    def c_copy(ch, i, src, dst, target):
        rcopy(src, dst, sc_s.at[ch], sc_r.at[ch, i], target)

    def c_wait(ch, i, ref):
        bytes_of(ref, sc_s.at[ch], sc_r.at[ch, i]).wait_recv()

    def last_copy(ch, src, kind, target):
        rcopy(src, last[LAST_DIRECT.index(ch)].at[kind, l], sc_s.at[ch], sc_r.at[ch, 2], target)

    def straight(ch, g):
        for zr, h in GROUPS[g]:
            last_copy(ch, cp[ch].at[zr, h], zr - 1, dev(c * 2 + h, y, lax.rem(z + zr, 4)))

    def c_far(ch):
        multiply(ch, 0)
        if ch in ALL_DIRECT:
            return straight(ch, 0)
        c_copy(ch, 0, cp[ch].at[2, 0], rsin[ch].at[0], dev_z(1))
        c_copy(ch, 1, cp[ch].at[2, 1], rsin[ch].at[1], dev_z(3))

    def c_near(ch):
        multiply(ch, 1)
        if ch in LAST_DIRECT:
            straight(ch, 1)
        else:
            c_copy(ch, 2, cp[ch].at[1, 1], rsin[ch].at[2], dev_z(1))
            c_copy(ch, 2, cp[ch].at[3, 0], rsin[ch].at[3], dev_z(3))

    def c_pre(ch):
        multiply(ch, 2)
        if ch in ALL_DIRECT:
            straight(ch, 2)

    def c_comb(ch, n):
        c_wait(ch, n, cp[ch].at[0, 0])
        rsout[ch][n] = rsin[ch][n] + cp[ch][1 + 2 * n, n]
        if ch in LAST_DIRECT:
            last_copy(ch, rsout[ch].at[n], 1, dev(c * 2 + n, y, lax.rem(z + 1 + 2 * n, 4)))
            return
        c_copy(ch, 2, rsout[ch].at[n], rsfin[ch].at[n], dev_z(1 + 2 * n))

    def c_own(ch):
        multiply(ch, 3)
        if ch in LAST_DIRECT:
            rcopy(cp[ch].at[0, 1 - l], last[LAST_DIRECT.index(ch)].at[3, l], sf_s.at[1 + LAST_DIRECT.index(ch)], sc_r.at[ch, 3], part)

    def out_half(ch, s, h):
        for t in range(CHUNKS[ch] // 128):
            col = s * HALF + (sum(CHUNKS[:ch]) + t * 128)
            out_ref[:, pl.ds(pl.multiple_of(col, 128), 128)] = ilv[ch][h, t].astype(BF16)

    def interleave(ch, h, value):
        for t in range(CHUNKS[ch] // 128):
            for p in range(2):
                half = value[p * 32 : p * 32 + 32, t * 128 : t * 128 + 128]
                ilv[ch][h, t, pl.ds(p, 32, stride=2), :] = half

    def c_final_direct(ch):
        at = LAST_DIRECT.index(ch)
        c_wait(ch, 2, cp[ch].at[pl.ds(0, 3 if ch in ALL_DIRECT else 2)])
        c_wait(ch, 3, cp[ch].at[0, 0])
        for n, s in enumerate((l, 1 - l)):
            value = last[at][3, s] if n else cp[ch][0, l]
            if ch in ALL_DIRECT:
                value += last[at][0, s] + last[at][2, s]
            else:
                value += last[at][2 * (1 - l), s]
            interleave(ch, n, value + last[at][1, s])
            out_half(ch, s, n)

    def c_final(ch):
        if ch in LAST_DIRECT:
            return c_final_direct(ch)
        c_wait(ch, 2, cp[ch].at[pl.ds(0, 2)])
        for h in range(2):
            value = cp[ch][0, h] + rsin[ch][3 - h] + rsfin[ch][h]
            interleave(ch, h, value)
        for t in range(CHUNKS[ch] // 128):
            fin_s[ch][:, pl.ds(t * 128, 128)] = ilv[ch][1 - l, t].astype(BF16)
        rcopy(fin_s[ch], fin_r[ch], sf_s.at[0], sc_r.at[ch, 3], part)
        out_half(ch, l, l)

    def c_last(ch):
        c_wait(ch, 3, fin_r[ch])
        col = (1 - l) * HALF + sum(CHUNKS[:ch])
        out_ref[:, pl.ds(pl.multiple_of(col, 128), CHUNKS[ch])] = fin_r[ch][...]

    steps = (
        ax, b_pair, b_own, b_other, b_mid, b_side, b_far, b_ready, a_prep, a_ring, a_fwd, a_ready,
        c_far, c_near, c_pre, c_comb, c_own, c_final, c_last,
    )
    for step, *where in ORDER:
        steps[step](*where)

    exchange[0].wait_send()
    for g in range(len(GROUPS)):
        bytes_of(abuf[g].at[pl.ds(0, 15)], sa_s.at[g], sa_r.at[g, 0]).wait_send()
    for ch in range(len(CHUNKS)):
        bytes_of(rbuf[ch].at[pl.ds(0, 1920)], sb_s.at[ch], sb_r.at[ch, 0]).wait_send()
        bytes_of(cp[ch].at[pl.ds(0, 3)], sc_s.at[ch], sc_r.at[ch, 0]).wait_send()
    for at, ch in enumerate(LAST_DIRECT):
        bytes_of(cp[ch].at[0, 0], sf_s.at[1 + at], sc_r.at[ch, 3]).wait_send()
    width = sum(CHUNKS[ch] for ch in range(len(CHUNKS)) if ch not in LAST_DIRECT)
    bytes_of(b_ref.at[pl.ds(0, 64), pl.ds(0, width)], sf_s.at[0], sc_r.at[0, 3]).wait_send()


def body(a_blocks, a_mask, a_row_ids, a_col_ids, b_matrix, b_mask):
    blocks = a_blocks.reshape(32, 2, 32, 128).transpose(0, 2, 1, 3).reshape(32, 64, 128)
    vmem = pl.BlockSpec(memory_space=pltpu.VMEM)
    hbm = pl.BlockSpec(memory_space=pltpu.HBM)
    n, groups = len(CHUNKS), len(GROUPS)
    rows = [128] * groups
    dma = pltpu.SemaphoreType.DMA
    scratch = [
        pltpu.SMEM((64,), jnp.int32),
        pltpu.SMEM((128,), jnp.int32),
        pltpu.SMEM((2, 32), jnp.int32),
        pltpu.SMEM((2, 48), jnp.int32),
        pltpu.VMEM((32, 64, 128), BF16),
        pltpu.VMEM((128, 3072), BF16),
        dma((6,)),
        pltpu.VMEM((8, 128), jnp.int32),
        pltpu.SMEM((8, 128), jnp.int32),
        pltpu.VMEM((64, 64, 128), BF16),
        pltpu.VMEM((8, 64, 128), F32),
        [pltpu.VMEM((2, 64, w), BF16) for w in CHUNKS],
        [pltpu.VMEM((3, m, 128), BF16) for m in rows],
        [pltpu.VMEM((16, m, 128), BF16) for m in rows],
        [pltpu.VMEM((8, 4, 64, w), BF16) for w in CHUNKS],
        [pltpu.VMEM((2048, w), BF16) for w in CHUNKS],
        [pltpu.VMEM((4, 2, 64, w), F32) for w in CHUNKS],
        [pltpu.VMEM((4, 64, w), F32) for w in CHUNKS],
        [pltpu.VMEM((2, 64, w), F32) for w in CHUNKS],
        [pltpu.VMEM((2, 64, w), F32) for w in CHUNKS],
        [pltpu.VMEM((2, w // 128, 64, 128), F32) for w in CHUNKS],
        [pltpu.VMEM((64, w), BF16) for w in CHUNKS],
        [pltpu.VMEM((64, w), BF16) for w in CHUNKS],
        [pltpu.VMEM((4, 2, 64, CHUNKS[ch]), F32) for ch in LAST_DIRECT],
        dma, dma, dma,
        dma((groups,)), dma((groups, 8)),
        dma((n,)), dma((n, 6)),
        dma((n,)), dma((n, 4)),
        dma((1 + len(LAST_DIRECT),)),
    ]
    return pl.pallas_call(
        kernel,
        out_shape=pltpu.VMEM((64, 3072), BF16),
        in_specs=[hbm] * 6,
        out_specs=vmem,
        scratch_shapes=scratch,
        compiler_params=pltpu.CompilerParams(collective_id=0, has_side_effects=True),
        name="contract",
    )(a_row_ids, a_col_ids, a_mask.T, b_mask, blocks, b_matrix)


def solution(mesh):
    return jax.shard_map(
        body,
        mesh=mesh,
        in_specs=(
            P("row", ("col", "depth"), None),
            P("row", ("col", "depth")),
            P(),
            P(),
            P(("row", "depth"), "col"),
            P(("row", "depth"), "col"),
        ),
        out_specs=P(("row", "depth"), "col"),
        check_vma=False,
    )
```
